32 devices in a mesh: dp: 1, ep: 32 (over z, y, x, core).
Axes of the slice: x: 2, y: 2, z: 4, core: 2. Of those that a mesh axis runs over, the one named last changes fastest.
Arguments:
- tokens: bfloat16 [256, 1024], P(('dp', 'ep')), may hold values from -6 to 6
- expert_ids: int32 [256, 8], P(('dp', 'ep')), may hold values from 0 to 31, all different within a row; in each aligned block of 8 rows (0 to 7, 8 to 15, ...) at most 4 rows name the same one
- gate_quant: int32 [256, 8], P(('dp', 'ep')), may hold values from 1 to 1024
- bucket_ids: int32 [256], P(('dp', 'ep')), may hold values from 0 to 15
- bucket_counts: int32 [16], replicated, may hold values from 0 to 512
- gate_weight: bfloat16 [32, 1024, 384], P('ep', 'dp'), may hold values from -0.1875 to 0.1875
- up_weight: bfloat16 [32, 1024, 384], P('ep', 'dp'), may hold values from -0.1875 to 0.1875
- down_weight: bfloat16 [32, 384, 1024], P('ep', 'dp'), may hold values from -0.3125 to 0.3125
- cotangent: bfloat16 [256, 1024], P(('dp', 'ep')), may hold values from -6 to 6
Outputs:
- layer_out: bfloat16 [256, 1024], P(('dp', 'ep'))
- token_grad: bfloat16 [256, 1024], P(('dp', 'ep'))
- gate_grad: float32 [32, 1024, 384], P('ep', 'dp')
- up_grad: float32 [32, 1024, 384], P('ep', 'dp')
- down_grad: float32 [32, 384, 1024], P('ep', 'dp')
The draws below stay inside these ranges and needn't reach their ends.
Inputs may be any that keep to these rules, and one draw needn't show every extreme that they name: `expert_ids`: each row names 8 different experts. Among the 8 rows of one device no expert is named by more than 4 rows, and in every draw some expert is named by exactly 4 rows of some device.
All inputs are finite; a program needn't handle non-finite values.
Results may differ from the reference program's by a relative error of at most 0.0085.
Values may be sent and summed in bfloat16 or wider, within the bound.
A program may use at most 64 MiB of HBM per device.

```python
import math
import jax
import jax.numpy as jnp
import numpy as np
from jax import lax

D = 1024
FF = 384
TOP = 8
BUCKETS = 16
TOK_DEV = 8
EXPERTS = 32
CAP = 4
TOKENS = 256
N_DP = 1
N_EP = 32


def touch_ends(values, rng, smallest, largest):
    place = [jax.random.randint(jax.random.fold_in(rng, axis), (), 0, length) for axis, length in enumerate(values.shape)]
    longest = values.shape.index(max(values.shape))
    next_to = place[:longest] + [(place[longest] + 1) % values.shape[longest]] + place[longest + 1:]
    return values.at[tuple(place)].set(smallest).at[tuple(next_to)].set(largest)


def level_of(key, dims, shards, least, largest):
    gain, own = 1.0, jax.random.fold_in(key, 6)
    for dim, parts in shards:
        heights = jnp.exp(jax.random.uniform(jax.random.fold_in(own, dim), (parts,), jnp.float32, least / len(shards), largest / len(shards)))
        gain = gain * jnp.repeat(heights, dims[dim] // parts).reshape([-1 if axis == dim else 1 for axis in range(len(dims))])
    return gain


def assign_block(own_key, own, number, rows, number_of, top, bound, skew):
    sequence = jax.random.permutation(own_key, number_of)
    heavy_load, ordinary = shares(number_of, rows * top, bound, skew, True), shares(number_of, rows * top, bound, skew, False)
    places = jnp.arange(number_of)

    def named(sizes, turn):
        used = int((sizes > 0).sum())
        fixed = max(1, used // 4)
        shifted = fixed + (places - fixed + turn * (used - fixed)) % max(1, number_of - fixed)
        return jnp.zeros((number_of,), jnp.int32).at[sequence[jnp.where(places < fixed, places, shifted)]].set(jnp.asarray(sizes, jnp.int32))

    sizes = jnp.where(number % 4 == 0, named(heavy_load, number // 4), named(ordinary, number - number // 4 - 1))
    mixed = jax.random.permutation(jax.random.fold_in(own, 3), number_of)
    donor, sink = mixed[0:number_of // 2 * 2:2], mixed[1:number_of // 2 * 2:2]
    room = jnp.minimum(sizes[donor] - 1, bound - sizes[sink]) // 2
    room = jnp.where((donor == sequence[0]) | (sink == sequence[0]) | (sizes[sink] == 0), 0, jnp.maximum(room, 0))
    shifted = jax.random.randint(jax.random.fold_in(own, 4), (number_of // 2,), 0, 1 << 20) % (room + 1)
    sizes = sizes.at[donor].add(-shifted).at[sink].add(shifted)
    items = jnp.searchsorted(jnp.cumsum(sizes), jnp.arange(rows * top), side="right").astype(jnp.int32)
    table = items.reshape(top, rows).T
    table = table[jax.random.permutation(jax.random.fold_in(own, 1), rows)]
    turn = jax.random.randint(jax.random.fold_in(own, 2), (rows, 1), 0, top)
    return jnp.take_along_axis(table, (jnp.arange(top)[None, :] + turn) % top, axis=1)


def shares(amount, total, bound, lean, full):
    weights = [(1 << 20) // math.isqrt(grade ** lean) + 1 for grade in range(1, amount + 1)]
    largest = bound if full else min(bound, max(-(-total // amount), total * weights[0] // sum(weights)))
    least = 1 if total - largest >= amount - 1 else 0
    counts, rest = [largest] + [least] * (amount - 1), total - largest - least * (amount - 1)
    while rest > 0:
        candidates = [i for i in range(1, amount) if counts[i] < largest] or [i for i in range(1, amount) if counts[i] < bound]
        whole, budget = sum([weights[i] for i in candidates]), rest
        for i in candidates:
            more = min(bound - counts[i], max(1, budget * weights[i] // whole), rest)
            counts[i] = counts[i] + more
            rest = rest - more
    return np.array(counts)


def gaussian(key, dims, width, bound, split=(), kind=jnp.bfloat16):
    loudness = level_of(key, dims, split, -0.22, 0.18) if split else 1.0
    entries = jax.random.normal(key, dims, jnp.float32) * width * loudness
    return jnp.minimum(jnp.maximum(entries, -bound), bound).astype(kind)


def setup_inputs(seed: int = 0) -> dict:
    key_of = jax.random.split(jax.random.key(seed), 10)
    tokens = gaussian(key_of[0], (TOKENS, D), 1.0, 6.0, ((0, 32),))
    expert_ids_keys = jax.random.split(jax.random.fold_in(key_of[1], 1), TOKENS // TOK_DEV)
    expert_ids_turns = jax.random.permutation(jax.random.fold_in(key_of[1], 3), TOKENS // TOK_DEV)
    expert_ids = jax.vmap(lambda own, number: assign_block(jax.random.fold_in(key_of[1], 2), own, number, TOK_DEV, EXPERTS, TOP, CAP, 2))(expert_ids_keys, expert_ids_turns).reshape((TOKENS, TOP))
    gate_quant = touch_ends(jax.random.randint(key_of[2], (TOKENS, TOP), 1, 1025), jax.random.fold_in(key_of[2], 1), 1, 1024).astype(jnp.int32)
    bucket_ids = touch_ends(jax.random.randint(key_of[3], (TOKENS,), 0, BUCKETS), jax.random.fold_in(key_of[3], 1), 0, BUCKETS - 1).astype(jnp.int32)
    bucket_counts = touch_ends(jax.random.randint(key_of[4], (BUCKETS,), 0, 513), jax.random.fold_in(key_of[4], 1), 0, 512).astype(jnp.int32)
    gate_weight = gaussian(key_of[5], (EXPERTS, D, FF), D ** -0.5, 0.1875, ((0, 32),))
    up_weight = gaussian(key_of[6], (EXPERTS, D, FF), D ** -0.5, 0.1875, ((0, 32),))
    down_weight = gaussian(key_of[7], (EXPERTS, FF, D), FF ** -0.5, 0.3125, ((0, 32),))
    cotangent = gaussian(key_of[8], (TOKENS, D), 1.0, 6.0, ((0, 32),))
    return {"tokens": tokens, "expert_ids": expert_ids, "gate_quant": gate_quant, "bucket_ids": bucket_ids, "bucket_counts": bucket_counts, "gate_weight": gate_weight, "up_weight": up_weight, "down_weight": down_weight, "cotangent": cotangent}


def silu_parts(pre_gate):
    sigmoid_val = jax.nn.sigmoid(pre_gate)
    return pre_gate * sigmoid_val, sigmoid_val * (1.0 + pre_gate * (1.0 - sigmoid_val))


def contract_rows(left_rows, right_rows):
    return lax.dot_general(left_rows, right_rows, (((0,), (0,)), ((), ())), preferred_element_type=jnp.float32)


def contract_cols(left_rows, right_rows):
    return lax.dot_general(left_rows, right_rows, (((1,), (1,)), ((), ())), preferred_element_type=jnp.float32)


def expert_forward(rows_in, gate_full, up_full, down_full):
    pre_gate = jnp.dot(rows_in, gate_full, preferred_element_type=jnp.float32)
    pre_up = jnp.dot(rows_in, up_full, preferred_element_type=jnp.float32)
    activation, derivative = silu_parts(pre_gate)
    hidden = (activation * pre_up).astype(jnp.bfloat16)
    expert_out = jnp.dot(hidden, down_full, preferred_element_type=jnp.float32).astype(jnp.bfloat16)
    return expert_out, (pre_up, activation, derivative, hidden)


def expert_backward(rows_in, scaled, saved, gate_full, up_full, down_full):
    pre_up, activation, derivative, hidden = saved
    hidden_grad = contract_cols(scaled, down_full)
    gate_pre = (hidden_grad * pre_up * derivative).astype(jnp.bfloat16)
    up_pre = (hidden_grad * activation).astype(jnp.bfloat16)
    slot_grad = (contract_cols(gate_pre, gate_full) + contract_cols(up_pre, up_full)).astype(jnp.bfloat16)
    return slot_grad, contract_rows(rows_in, gate_pre), contract_rows(rows_in, up_pre), contract_rows(hidden, scaled)


def slot_table(flat_ids, experts, slot_cap):
    total_pairs = flat_ids.shape[0]
    onehot = (flat_ids[:, None] == jnp.arange(experts, dtype=jnp.int32)[None, :]).astype(jnp.int32)
    before = jnp.cumsum(onehot, axis=0) - onehot
    position = jnp.sum(before * onehot, axis=1)
    slot_of = (flat_ids * slot_cap + position).astype(jnp.int32)
    lookup = jnp.full((experts * slot_cap,), total_pairs, jnp.int32)
    lookup = lookup.at[slot_of].set(jnp.arange(total_pairs, dtype=jnp.int32))
    return lookup, slot_of


def reference(tokens, expert_ids, gate_quant, bucket_ids, bucket_counts, gate_weight, up_weight, down_weight, cotangent):
    experts = gate_weight.shape[0]
    top_count = expert_ids.shape[1]
    group_size = N_EP * TOK_DEV
    slot_cap = N_EP * CAP
    model_width = tokens.shape[1]
    gate_share = gate_quant.astype(jnp.float32) / 1024.0
    token_scale = 64.0 / (64.0 + bucket_counts[bucket_ids].astype(jnp.float32))
    scaled_share = gate_share * token_scale[:, None]
    out_parts = []
    grad_parts = []
    totals = None
    for group_idx in range(N_DP):
        first_row = group_idx * group_size
        group_tokens = tokens[first_row:first_row + group_size]
        group_cot = cotangent[first_row:first_row + group_size]
        flat_ids = expert_ids[first_row:first_row + group_size].reshape(-1)
        gate_flat = gate_share[first_row:first_row + group_size].reshape(-1)
        scaled_flat = scaled_share[first_row:first_row + group_size].reshape(-1)
        lookup, slot_of = slot_table(flat_ids, experts, slot_cap)
        total_pairs = flat_ids.shape[0]

        def per_expert(running, expert_item):
            out_acc, grad_acc = running
            pair_index, gate_full, up_full, down_full = expert_item
            is_live = pair_index < total_pairs
            safe_index = jnp.where(is_live, pair_index, 0).astype(jnp.int32)
            source_row = (safe_index // top_count).astype(jnp.int32)
            rows_in = jnp.where(is_live[:, None], group_tokens[source_row], jnp.zeros((), jnp.bfloat16)).astype(jnp.bfloat16)
            gate_slot = jnp.where(is_live, gate_flat[safe_index], jnp.zeros((), jnp.float32))
            scale_slot = jnp.where(is_live, scaled_flat[safe_index], jnp.zeros((), jnp.float32))
            scaled = (scale_slot[:, None] * group_cot[source_row].astype(jnp.float32)).astype(jnp.bfloat16)
            expert_out, saved = expert_forward(rows_in, gate_full, up_full, down_full)
            slot_grad, grad_gate, grad_up, grad_down = expert_backward(rows_in, scaled, saved, gate_full, up_full, down_full)
            out_acc = out_acc.at[source_row].add(gate_slot[:, None] * expert_out.astype(jnp.float32))
            grad_acc = grad_acc.at[source_row].add(jnp.where(is_live[:, None], slot_grad.astype(jnp.float32), jnp.zeros((), jnp.float32)))
            return (out_acc, grad_acc), (grad_gate.astype(jnp.bfloat16), grad_up.astype(jnp.bfloat16), grad_down.astype(jnp.bfloat16))

        start_acc = (jnp.zeros((group_size, model_width), jnp.float32), jnp.zeros((group_size, model_width), jnp.float32))
        stacked = (lookup.reshape(experts, slot_cap), gate_weight, up_weight, down_weight)
        (out_acc, grad_acc), partials = lax.scan(per_expert, start_acc, stacked)
        out_parts.append(out_acc.astype(jnp.bfloat16))
        grad_parts.append(grad_acc.astype(jnp.bfloat16))
        widened = tuple(part.astype(jnp.float32) for part in partials)
        if totals is None:
            totals = widened
        else:
            totals = tuple(acc + part for acc, part in zip(totals, widened))
    layer_out = jnp.concatenate(out_parts, axis=0)
    token_grad = jnp.concatenate(grad_parts, axis=0)
    return (layer_out, token_grad, totals[0], totals[1], totals[2])
```

```python
import functools
import jax
import jax.numpy as jnp
from jax import lax
from jax.experimental import pallas as pl
from jax.experimental.pallas import tpu as pltpu
from jax.sharding import PartitionSpec as P

BF = jnp.bfloat16
F32 = jnp.float32
MESH = pl.DeviceIdType.MESH


def dot(a, b, ca, cb):
    return lax.dot_general(a, b, (((ca,), (cb,)), ((), ())), preferred_element_type=F32)


def kernel(
    n_ep, lanes, n_sem,
    bid_ref, bcnt_ref, tok_ref, ids_ref, quant_ref, cot_ref, wg_hbm, wu_hbm, wd_hbm,
    lo_ref, tg_ref, gg_ref, gu_ref, gd_ref,
    gat, meta_f, wg, wu, wd, og, pa, pb, r1a, r1b, s1a, s1b, r2a, r2b, s2a, s2b, r3a, r3b, s3a, s3b, r4a, r4b,
    send_sems, recv_sems, w_sems,
):
    rows, width = tok_ref.shape
    top = ids_ref.shape[1]
    nz = n_ep // 8
    R = rows
    half = 4 * R
    group = 8 * R
    me = lax.axis_index("ep")
    z = me // 8
    rest = me % 8
    y, x, c = rest // 4, (rest // 2) % 2, rest % 2
    base = z * 8
    core_nbr = base + y * 4 + x * 2 + (1 - c)
    x_nbr = base + y * 4 + (1 - x) * 2 + c
    y_nbr = base + (1 - y) * 4 + x * 2 + c
    z_nbr = [None] + [lax.rem(z + k, nz) * 8 + rest for k in range(1, nz)]
    partners = [core_nbr, x_nbr, y_nbr] + z_nbr[1:]

    w_copies = [
        pltpu.make_async_copy(src.at[0], dst, w_sems.at[i])
        for i, (src, dst) in enumerate(((wg_hbm, wg), (wu_hbm, wu), (wd_hbm, wd)))
    ]
    for cp in w_copies:
        cp.start()

    barrier = pltpu.get_barrier_semaphore()
    for d in partners:
        pl.semaphore_signal(barrier, inc=1, device_id={"ep": d}, device_id_type=MESH)

    lane = lax.broadcasted_iota(jnp.int32, (rows, lanes), 1)
    row = lax.broadcasted_iota(jnp.int32, (rows, lanes), 0)
    count = jnp.zeros((rows, lanes), jnp.int32)
    for t in range(rows):
        count = jnp.where(row == t, bcnt_ref[bid_ref[t]], count)
    ids = ids_ref[...]
    quant = quant_ref[...]
    meta = jnp.where(lane == 2 * n_ep, count >> 5, jnp.where(lane == 2 * n_ep + 1, count & 31, 0))
    for k in range(top):
        ik = ids[:, k:k + 1]
        qk = quant[:, k:k + 1]
        meta = meta + jnp.where(lane == ik, qk >> 5, 0) + jnp.where(lane == ik + n_ep, qk & 31, 0)
    a_cols = slice(0, width + lanes)
    b_cols = slice(width + lanes, 2 * width + lanes)
    all_cols = slice(0, 2 * width + lanes)
    gat[0:R, 0:width] = tok_ref[...]
    gat[0:R, width:width + lanes] = meta.astype(F32).astype(BF)
    gat[0:R, b_cols] = cot_ref[...]

    def slot(k, cc, yy, xx):
        return k * group + cc * half + yy * 2 * R + xx * R

    pl.semaphore_wait(barrier, len(partners))

    pending = []
    counter = [0]

    def send(src, dst, target):
        i = counter[0]
        counter[0] += 1
        cp = pltpu.make_async_remote_copy(
            src_ref=src, dst_ref=dst, send_sem=send_sems.at[i], recv_sem=recv_sems.at[i],
            device_id={"ep": target}, device_id_type=MESH,
        )
        cp.start()
        pending.append(cp)
        return cp

    def g(s, cols):
        return gat.at[s:s + R, cols]

    zc = {}
    xc, yc, cc, dac, dbc = {}, {}, {}, {}, {}

    def spread(k):
        s = slot(k, 0, 0, 0)
        xc[k] = send(g(s, all_cols), g(slot(k, 0, 0, 1), all_cols), x_nbr)
        yc[k] = send(g(s, all_cols), g(slot(k, 0, 1, 0), all_cols), y_nbr)
        cc[k, 0, 0] = send(g(s, all_cols), g(slot(k, 1, 0, 0), all_cols), core_nbr)

    def diag(k):
        yc[k].wait_recv()
        s = slot(k, 0, 1, 0)
        dac[k] = send(g(s, a_cols), g(slot(k, 0, 1, 1), a_cols), x_nbr)
        cc[k, 1, 0] = send(g(s, all_cols), g(slot(k, 1, 1, 0), all_cols), core_nbr)
        xc[k].wait_recv()
        s = slot(k, 0, 0, 1)
        dbc[k] = send(g(s, b_cols), g(slot(k, 0, 1, 1), b_cols), y_nbr)
        cc[k, 0, 1] = send(g(s, all_cols), g(slot(k, 1, 0, 1), all_cols), core_nbr)

    for k in range(1, nz):
        zc[nz - k] = send(g(0, all_cols), g(slot(nz - k, 0, 0, 0), all_cols), z_nbr[k])
    spread(0)
    diag(0)
    for k in range(1, nz):
        zc[k].wait_recv()
        spread(k)
    for k in range(1, nz):
        diag(k)
    for k in range(nz):
        dac[k].wait_recv()
        dbc[k].wait_recv()
        s = slot(k, 0, 1, 1)
        cc[k, 1, 1] = send(g(s, all_cols), g(slot(k, 1, 1, 1), all_cols), core_nbr)
    for cp in w_copies:
        cp.wait()
    for k in range(nz):
        for yy in range(2):
            for xx in range(2):
                cc[k, yy, xx].wait_recv()

    toks = gat[:, 0:width]
    m = gat[:, width:width + lanes].astype(F32)
    ml = lax.broadcasted_iota(jnp.int32, m.shape, 1)
    share = jnp.sum(jnp.where(ml == me, m * 32.0, jnp.where(ml == me + n_ep, m, 0.0)), axis=1, keepdims=True) / 1024.0
    cnt = jnp.sum(jnp.where(ml == 2 * n_ep, m * 32.0, jnp.where(ml == 2 * n_ep + 1, m, 0.0)), axis=1, keepdims=True)
    scale = share * (64.0 / (64.0 + cnt))
    pre_gate = dot(toks, wg[...], 1, 0)
    pre_up = dot(toks, wu[...], 1, 0)
    sig = jax.nn.sigmoid(pre_gate)
    act = pre_gate * sig
    hidden = (act * pre_up).astype(BF)
    pa[...] = (share * dot(hidden, wd[...], 1, 0)).astype(BF)
    order = list(range(1, nz)) + [0]

    def send1(p, r1):
        return {
            k: send(p.at[k * group + half:(k + 1) * group, :], r1.at[k], core_nbr) for k in order
        }

    c1a = send1(pa, r1a)
    og[...] = (scale * gat[:, b_cols].astype(F32)).astype(BF)
    hg = dot(og[...], wd[...], 1, 1)
    gate_pre = (hg * pre_up * (sig * (1.0 + pre_gate * (1.0 - sig)))).astype(BF)
    up_pre = (hg * act).astype(BF)
    pb[...] = (dot(gate_pre, wg[...], 1, 1) + dot(up_pre, wu[...], 1, 1)).astype(BF)
    c1b = send1(pb, r1b)

    def part(ref, k, yy, xx):
        s = slot(k, 0, yy, xx)
        return ref[s:s + R, :].astype(F32)

    def sub(ref, k, yy, xx):
        s = yy * 2 * R + xx * R
        return ref[k, s:s + R, :].astype(F32)

    def one(k, yy, xx, p, r1):
        return part(p, k, yy, xx) + sub(r1, k, yy, xx)

    def step2(p, c1, r1, s1, r2, target, at):
        out = {}
        for k in order:
            c1[k].wait_recv()
            for i in range(2):
                yy, xx = at(1, i)
                s1[k, i * R:(i + 1) * R, :] = one(k, yy, xx, p, r1).astype(BF)
            out[k] = send(s1.at[k], r2.at[k], target)
        return out

    def step3(p, r1, c2, r2, s2, r3, target, at):
        out = {}
        for k in order:
            c2[k].wait_recv()
            yy, xx = at(0, 1)
            s2[k] = (one(k, yy, xx, p, r1) + r2[k, R:2 * R, :].astype(F32)).astype(BF)
            out[k] = send(s2.at[k], r3.at[k], target)
        return out

    def local(k, p, r1, r2, r3):
        return one(k, 0, 0, p, r1) + r2[k, 0:R, :].astype(F32) + r3[k].astype(F32)

    def step4(p, r1, r2, c3, r3, s3, r4):
        out = {}
        for k in order:
            c3[k].wait_recv()
            if k:
                s3[k] = local(k, p, r1, r2, r3).astype(BF)
                out[nz - k] = send(s3.at[k], r4.at[nz - k], z_nbr[k])
        return out

    def finish(p, r1, r2, r3, c4, r4, out_ref):
        total = local(0, p, r1, r2, r3)
        for k in range(1, nz):
            c4[k].wait_recv()
            total = total + r4[k].astype(F32)
        out_ref[...] = total.astype(BF)

    at_a = lambda far, i: (i, far)
    at_b = lambda far, i: (far, i)
    c2a = step2(pa, c1a, r1a, s1a, r2a, x_nbr, at_a)
    c2b = step2(pb, c1b, r1b, s1b, r2b, y_nbr, at_b)
    gg_ref[0] = dot(toks, gate_pre, 0, 0).astype(gg_ref.dtype)
    c3a = step3(pa, r1a, c2a, r2a, s2a, r3a, y_nbr, at_a)
    c3b = step3(pb, r1b, c2b, r2b, s2b, r3b, x_nbr, at_b)
    gu_ref[0] = dot(toks, up_pre, 0, 0).astype(gu_ref.dtype)
    c4a = step4(pa, r1a, r2a, c3a, r3a, s3a, r4a)
    c4b = step4(pb, r1b, r2b, c3b, r3b, s3b, r4b)
    gd_ref[0] = dot(hidden, og[...], 0, 0).astype(gd_ref.dtype)
    finish(pa, r1a, r2a, r3a, c4a, r4a, lo_ref)
    finish(pb, r1b, r2b, r3b, c4b, r4b, tg_ref)
    for cp in pending:
        cp.wait_send()
    assert counter[0] == n_sem


def per_device(
    tokens, expert_ids, gate_quant, bucket_ids, bucket_counts,
    gate_weight, up_weight, down_weight, cotangent,
):
    n_ep = lax.axis_size("ep")
    n_dp = lax.axis_size("dp")
    rows, width = tokens.shape
    if n_dp > 1:
        gate_weight, up_weight, down_weight = (
            lax.all_gather(w, "dp", axis=1, tiled=True)
            for w in (gate_weight, up_weight, down_weight)
        )
    ff = gate_weight.shape[2]
    nz = n_ep // 8
    lanes = -(-(2 * n_ep + 2) // 128) * 128
    total = n_ep * rows
    n_sem = (nz - 1) + 3 * nz + 4 * nz + nz + 2 * nz + 2 * nz + 2 * nz + 2 * (nz - 1)
    vm = pl.BlockSpec(memory_space=pltpu.VMEM)
    sm = pl.BlockSpec(memory_space=pltpu.SMEM)
    hb = pl.BlockSpec(memory_space=pltpu.HBM)
    V = pltpu.VMEM
    pair = lambda shape: [V(shape, BF), V(shape, BF)]
    outs = pl.pallas_call(
        functools.partial(kernel, n_ep, lanes, n_sem),
        out_shape=(
            jax.ShapeDtypeStruct((rows, width), BF),
            jax.ShapeDtypeStruct((rows, width), BF),
            jax.ShapeDtypeStruct((1, width, ff), BF),
            jax.ShapeDtypeStruct((1, width, ff), BF),
            jax.ShapeDtypeStruct((1, ff, width), BF),
        ),
        in_specs=[sm, sm, vm, vm, vm, vm, hb, hb, hb],
        out_specs=[vm] * 5,
        scratch_shapes=[
            V((total, 2 * width + lanes), BF),
            V((8, 128), F32),
            V((width, ff), BF),
            V((width, ff), BF),
            V((ff, width), BF),
            V((total, width), BF),
            *pair((total, width)),
            *pair((nz, 4 * rows, width)),
            *pair((nz, 2 * rows, width)),
            *pair((nz, 2 * rows, width)),
            *pair((nz, rows, width)),
            *pair((nz, rows, width)),
            *pair((nz, rows, width)),
            *pair((nz, rows, width)),
            pltpu.SemaphoreType.DMA((n_sem,)),
            pltpu.SemaphoreType.DMA((n_sem,)),
            pltpu.SemaphoreType.DMA((3,)),
        ],
        compiler_params=pltpu.CompilerParams(collective_id=0, has_side_effects=True, vmem_limit_bytes=60 * 1024 * 1024),
    )(bucket_ids, bucket_counts, tokens, expert_ids, gate_quant, cotangent, gate_weight, up_weight, down_weight)
    layer_out, token_grad, gg, gu, gd = outs
    if n_dp > 1:
        gg, gu, gd = (
            lax.psum_scatter(v, "dp", scatter_dimension=1, tiled=True) for v in (gg, gu, gd)
        )
    return (layer_out, token_grad, gg.astype(F32), gu.astype(F32), gd.astype(F32))


def solution(mesh):
    placed = (
        P(("dp", "ep"), None), P(("dp", "ep"), None), P(("dp", "ep"), None), P(("dp", "ep")), P(),
        P("ep", "dp", None), P("ep", "dp", None), P("ep", "dp", None), P(("dp", "ep"), None),
    )
    return jax.shard_map(
        per_device, mesh=mesh, in_specs=placed,
        out_specs=(
            P(("dp", "ep"), None), P(("dp", "ep"), None),
            P("ep", "dp", None), P("ep", "dp", None), P("ep", "dp", None),
        ),
        check_vma=False,
    )
```

```python
import functools
import jax
import jax.numpy as jnp
from jax import lax
from jax.experimental import pallas as pl
from jax.experimental.pallas import tpu as pltpu
from jax.sharding import PartitionSpec as P

BF = jnp.bfloat16
F32 = jnp.float32
MESH = pl.DeviceIdType.MESH


def dot(a, b, ca, cb):
    return lax.dot_general(a, b, (((ca,), (cb,)), ((), ())), preferred_element_type=F32)


def kernel(
    n_ep, lanes, n_sem,
    bid_hbm, bcnt_hbm, tok_hbm, ids_hbm, quant_hbm, cot_hbm, wg_hbm, wu_hbm, wd_hbm,
    lo_ref, tg_ref, gg_hbm, gu_hbm, gd_hbm,
    gat, wg, wu, wd, og, pa, pb, r1a, r1b, s1a, s1b, r2a, r2b, s2a, s2b, r3a, r3b, s3a, s3b, r4a, r4b,
    ids_v, quant_v, bid_s, bcnt_s, gg, gu, gd,
    send_sems, recv_sems, w_sems, i_sems, o_sems,
):
    R, width = tok_hbm.shape
    top = ids_hbm.shape[1]
    nz = n_ep // 8
    group = 8 * R
    me = lax.axis_index("ep")
    z = me // 8
    rest = me % 8
    y, x, c = rest // 4, (rest // 2) % 2, rest % 2
    base = z * 8
    core_nbr = base + y * 4 + x * 2 + (1 - c)
    x_nbr = base + y * 4 + (1 - x) * 2 + c
    y_nbr = base + (1 - y) * 4 + x * 2 + c
    near = [jnp.where(z < nz // 2, i, nz - i) for i in range(1, nz)]
    far = near[::-1]

    def z_at(k):
        return lax.rem(z + k, nz) * 8 + rest

    a_cols = slice(0, width + lanes)
    b_cols = slice(width + lanes, 2 * width + lanes)
    cols = {"a": a_cols, "b": b_cols}

    i_copies = [
        pltpu.make_async_copy(src, dst, i_sems.at[i])
        for i, (src, dst) in enumerate((
            (bid_hbm, bid_s), (bcnt_hbm, bcnt_s), (ids_hbm, ids_v), (quant_hbm, quant_v),
            (tok_hbm, gat.at[0, 0:R, 0:width]), (cot_hbm, gat.at[0, 0:R, b_cols]),
        ))
    ]
    for cp in i_copies:
        cp.start()
    w_copies = [
        pltpu.make_async_copy(src.at[0], dst, w_sems.at[i])
        for i, (src, dst) in enumerate(((wg_hbm, wg), (wu_hbm, wu), (wd_hbm, wd)))
    ]
    for cp in w_copies:
        cp.start()
    barrier = pltpu.get_barrier_semaphore()
    for d in [z_at(k) for k in range(1, nz)] + [core_nbr, x_nbr, y_nbr]:
        pl.semaphore_signal(barrier, inc=1, device_id={"ep": d}, device_id_type=MESH)
    for cp in i_copies:
        cp.wait()

    lane = lax.broadcasted_iota(jnp.int32, (R, lanes), 1)
    row = lax.broadcasted_iota(jnp.int32, (R, lanes), 0)
    count = jnp.zeros((R, lanes), jnp.int32)
    for t in range(R):
        count = jnp.where(row == t, bcnt_s[bid_s[t]], count)
    ids = ids_v[...]
    quant = quant_v[...]
    meta = jnp.where(lane == 2 * n_ep, count >> 5, jnp.where(lane == 2 * n_ep + 1, count & 31, 0))
    for k in range(top):
        ik = ids[:, k:k + 1]
        qk = quant[:, k:k + 1]
        meta = meta + jnp.where(lane == ik, qk >> 5, 0) + jnp.where(lane == ik + n_ep, qk & 31, 0)
    gat[0, 0:R, width:width + lanes] = meta.astype(F32).astype(BF)
    pl.semaphore_wait(barrier, nz + 2)

    pending = []
    bases = {}

    def index(name, k):
        if name not in bases:
            bases[name] = len(bases) * nz
        return bases[name] + k

    def send(name, src, dst, target, k):
        i = index(name, k)
        cp = pltpu.make_async_remote_copy(
            src_ref=src, dst_ref=dst, send_sem=send_sems.at[i], recv_sem=recv_sems.at[i],
            device_id={"ep": target}, device_id_type=MESH,
        )
        cp.start()
        pending.append(cp)

    def landed(name, dst, k):
        i = index(name, k)
        pltpu.make_async_remote_copy(
            src_ref=dst, dst_ref=dst, send_sem=send_sems.at[i], recv_sem=recv_sems.at[i],
            device_id={"ep": core_nbr}, device_id_type=MESH,
        ).wait_recv()

    def blk(h, k, cc, yy, xx):
        s = cc * 4 * R + yy * 2 * R + xx * R
        return gat.at[k, s:s + R, cols[h]]

    def to_x(h, k):
        send("x" + h, blk(h, k, 0, 0, 0), blk(h, k, 0, 0, 1), x_nbr, k)

    def to_y(h, k):
        send("y" + h, blk(h, k, 0, 0, 0), blk(h, k, 0, 1, 0), y_nbr, k)

    def to_core(h, k, yy, xx):
        send("c%d%d" % (yy, xx) + h, blk(h, k, 0, yy, xx), blk(h, k, 1, yy, xx), core_nbr, k)

    def spread(h, k):
        if h == "a":
            to_y(h, k)
            to_x(h, k)
        else:
            to_x(h, k)
            to_y(h, k)
        to_core(h, k, 0, 0)

    def start_z(h):
        for k in far:
            send("z" + h, blk(h, 0, 0, 0, 0), blk(h, nz - k, 0, 0, 0), z_at(k), nz - k)

    def pass_z(h, k):
        landed("z" + h, blk(h, k, 0, 0, 0), k)
        spread(h, k)

    def pass_xy(h, k):
        if h == "a":
            landed("y" + h, blk(h, k, 0, 1, 0), k)
            send("d" + h, blk(h, k, 0, 1, 0), blk(h, k, 0, 1, 1), x_nbr, k)
            to_core(h, k, 1, 0)
            landed("x" + h, blk(h, k, 0, 0, 1), k)
            to_core(h, k, 0, 1)
        else:
            landed("x" + h, blk(h, k, 0, 0, 1), k)
            send("d" + h, blk(h, k, 0, 0, 1), blk(h, k, 0, 1, 1), y_nbr, k)
            to_core(h, k, 0, 1)
            landed("y" + h, blk(h, k, 0, 1, 0), k)
            to_core(h, k, 1, 0)

    def pass_d(h, k):
        landed("d" + h, blk(h, k, 0, 1, 1), k)
        to_core(h, k, 1, 1)

    def all_core(h):
        for k in range(nz):
            for yy in range(2):
                for xx in range(2):
                    landed("c%d%d" % (yy, xx) + h, blk(h, k, 1, yy, xx), k)

    start_z("a")
    spread("a", 0)
    start_z("b")
    spread("b", 0)
    pass_xy("a", 0)
    for k in near:
        pass_z("a", k)
    pass_xy("b", 0)
    for k in near:
        pass_z("b", k)
    for k in near:
        pass_xy("a", k)
    pass_d("a", 0)
    for k in near:
        pass_xy("b", k)
    for k in near:
        pass_d("a", k)
    for cp in w_copies:
        cp.wait()
    all_core("a")

    total = n_ep * R
    toks = gat[:, :, 0:width].reshape(total, width)
    m = gat[:, :, width:width + lanes].reshape(total, lanes).astype(F32)
    ml = lax.broadcasted_iota(jnp.int32, m.shape, 1)
    share = jnp.sum(jnp.where(ml == me, m * 32.0, jnp.where(ml == me + n_ep, m, 0.0)), axis=1, keepdims=True) / 1024.0
    cnt = jnp.sum(jnp.where(ml == 2 * n_ep, m * 32.0, jnp.where(ml == 2 * n_ep + 1, m, 0.0)), axis=1, keepdims=True)
    scale = share * (64.0 / (64.0 + cnt))
    pre_gate = dot(toks, wg[...], 1, 0)
    pre_up = dot(toks, wu[...], 1, 0)
    pass_d("b", 0)
    for k in near:
        pass_d("b", k)
    sig = jax.nn.sigmoid(pre_gate)
    act = pre_gate * sig
    hidden = (act * pre_up).astype(BF)
    pa[...] = (share * dot(hidden, wd[...], 1, 0)).astype(BF).reshape(pa.shape)
    order = far + [0]

    def send1(h, p, r1):
        for k in order:
            send("r1" + h, p.at[k, 4 * R:8 * R, :], r1.at[k], core_nbr, k)

    send1("a", pa, r1a)
    all_core("b")
    og[...] = (scale * gat[:, :, b_cols].reshape(total, width).astype(F32)).astype(BF)
    hg = dot(og[...], wd[...], 1, 1)
    gate_pre = (hg * pre_up * (sig * (1.0 + pre_gate * (1.0 - sig)))).astype(BF)
    up_pre = (hg * act).astype(BF)

    def sub(ref, k, yy, xx):
        s = yy * 2 * R + xx * R
        return ref[k, s:s + R, :].astype(F32)

    def one(k, yy, xx, p, r1):
        return sub(p, k, yy, xx) + sub(r1, k, yy, xx)

    def step2(h, p, r1, s1, r2, target, at):
        for k in order:
            landed("r1" + h, r1.at[k], k)
            for i in range(2):
                yy, xx = at(1, i)
                s1[k, i * R:(i + 1) * R, :] = one(k, yy, xx, p, r1).astype(BF)
            send("r2" + h, s1.at[k], r2.at[k], target, k)

    def step3(h, p, r1, r2, s2, r3, target, at):
        for k in order:
            landed("r2" + h, r2.at[k], k)
            yy, xx = at(0, 1)
            s2[k] = (one(k, yy, xx, p, r1) + r2[k, R:2 * R, :].astype(F32)).astype(BF)
            send("r3" + h, s2.at[k], r3.at[k], target, k)

    def local(k, p, r1, r2, r3):
        return one(k, 0, 0, p, r1) + r2[k, 0:R, :].astype(F32) + r3[k].astype(F32)

    def step4(h, p, r1, r2, r3, s3, r4):
        for k in far:
            landed("r3" + h, r3.at[k], k)
            s3[k] = local(k, p, r1, r2, r3).astype(BF)
            send("r4" + h, s3.at[k], r4.at[nz - k], z_at(k), nz - k)
        landed("r3" + h, r3.at[0], 0)

    def finish(h, p, r1, r2, r3, r4, out_ref):
        acc = local(0, p, r1, r2, r3)
        for k in near:
            landed("r4" + h, r4.at[k], k)
            acc = acc + r4[k].astype(F32)
        out_ref[...] = acc.astype(BF)

    at_a = lambda away, i: (i, away)
    at_b = lambda away, i: (away, i)
    o_copies = []

    def weight_grad(left, right, buf, out):
        buf[...] = dot(left, right, 0, 0).astype(BF)
        cp = pltpu.make_async_copy(buf, out.at[0], o_sems.at[len(o_copies)])
        cp.start()
        o_copies.append(cp)

    step2("a", pa, r1a, s1a, r2a, x_nbr, at_a)
    pb[...] = (dot(gate_pre, wg[...], 1, 1) + dot(up_pre, wu[...], 1, 1)).astype(BF).reshape(pb.shape)
    send1("b", pb, r1b)
    weight_grad(toks, gate_pre, gg, gg_hbm)
    step2("b", pb, r1b, s1b, r2b, y_nbr, at_b)
    step3("a", pa, r1a, r2a, s2a, r3a, y_nbr, at_a)
    weight_grad(toks, up_pre, gu, gu_hbm)
    step3("b", pb, r1b, r2b, s2b, r3b, x_nbr, at_b)
    step4("a", pa, r1a, r2a, r3a, s3a, r4a)
    weight_grad(hidden, og[...], gd, gd_hbm)
    step4("b", pb, r1b, r2b, r3b, s3b, r4b)
    finish("a", pa, r1a, r2a, r3a, r4a, lo_ref)
    finish("b", pb, r1b, r2b, r3b, r4b, tg_ref)
    for cp in pending:
        cp.wait_send()
    for cp in o_copies:
        cp.wait()
    assert len(bases) * nz == n_sem


def widen(parts, lo_in, tg_in, gg_in, gu_in, gd_in, lo, tg, gg, gu, gd, gb, ub, db, gf, uf, df, in_sems, out_sems):
    lo[...] = lo_in[...]
    tg[...] = tg_in[...]
    work = []
    for w, (src, mid, wide, dst) in enumerate(((gg_in, gb, gf, gg), (gu_in, ub, uf, gu), (gd_in, db, df, gd))):
        rows = mid.shape[0] // parts
        for i in range(parts):
            at = slice(i * rows, (i + 1) * rows)
            n = w * parts + i
            cp = pltpu.make_async_copy(src.at[0, at, :], mid.at[at, :], in_sems.at[n])
            cp.start()
            out = pltpu.make_async_copy(wide.at[at, :], dst.at[0, at, :], out_sems.at[n])
            work.append((cp, out, mid, wide, at))
    for cp, out, mid, wide, at in work:
        cp.wait()
        wide[at, :] = mid[at, :].astype(F32)
        out.start()
    for item in work:
        item[1].wait()


def per_device(
    tokens, expert_ids, gate_quant, bucket_ids, bucket_counts,
    gate_weight, up_weight, down_weight, cotangent,
):
    n_ep = lax.axis_size("ep")
    n_dp = lax.axis_size("dp")
    rows, width = tokens.shape
    if n_dp > 1:
        gate_weight, up_weight, down_weight = (
            lax.all_gather(w, "dp", axis=1, tiled=True)
            for w in (gate_weight, up_weight, down_weight)
        )
    ff = gate_weight.shape[2]
    nz = n_ep // 8
    lanes = -(-(2 * n_ep + 2) // 128) * 128
    n_sem = 24 * nz
    vm = pl.BlockSpec(memory_space=pltpu.VMEM)
    hb = pl.BlockSpec(memory_space=pltpu.HBM)
    V = pltpu.VMEM
    pair = lambda shape: [V(shape, BF), V(shape, BF)]
    outs = pl.pallas_call(
        functools.partial(kernel, n_ep, lanes, n_sem),
        out_shape=(
            jax.ShapeDtypeStruct((rows, width), BF),
            jax.ShapeDtypeStruct((rows, width), BF),
            jax.ShapeDtypeStruct((1, width, ff), BF),
            jax.ShapeDtypeStruct((1, width, ff), BF),
            jax.ShapeDtypeStruct((1, ff, width), BF),
        ),
        in_specs=[hb] * 9,
        out_specs=[vm, vm, hb, hb, hb],
        scratch_shapes=[
            V((nz, 8 * rows, 2 * width + lanes), BF),
            V((width, ff), BF),
            V((width, ff), BF),
            V((ff, width), BF),
            V((n_ep * rows, width), BF),
            *pair((nz, 8 * rows, width)),
            *pair((nz, 4 * rows, width)),
            *pair((nz, 2 * rows, width)),
            *pair((nz, 2 * rows, width)),
            *pair((nz, rows, width)),
            *pair((nz, rows, width)),
            *pair((nz, rows, width)),
            *pair((nz, rows, width)),
            V(expert_ids.shape, jnp.int32),
            V(gate_quant.shape, jnp.int32),
            pltpu.SMEM(bucket_ids.shape, jnp.int32),
            pltpu.SMEM(bucket_counts.shape, jnp.int32),
            V((width, ff), BF),
            V((width, ff), BF),
            V((ff, width), BF),
            pltpu.SemaphoreType.DMA((n_sem,)),
            pltpu.SemaphoreType.DMA((n_sem,)),
            pltpu.SemaphoreType.DMA((3,)),
            pltpu.SemaphoreType.DMA((6,)),
            pltpu.SemaphoreType.DMA((3,)),
        ],
        compiler_params=pltpu.CompilerParams(collective_id=0, has_side_effects=True, vmem_limit_bytes=60 * 1024 * 1024),
    )(bucket_ids, bucket_counts, tokens, expert_ids, gate_quant, cotangent, gate_weight, up_weight, down_weight)
    layer_out, token_grad, gg, gu, gd = outs
    if n_dp > 1:
        gg, gu, gd = (
            lax.psum_scatter(v, "dp", scatter_dimension=1, tiled=True) for v in (gg, gu, gd)
        )
    parts = 2
    wide = [jax.ShapeDtypeStruct(v.shape, F32) for v in (gg, gu, gd)]
    return pl.pallas_call(
        functools.partial(widen, parts),
        out_shape=(
            jax.ShapeDtypeStruct((rows, width), BF),
            jax.ShapeDtypeStruct((rows, width), BF),
            *wide,
        ),
        in_specs=[vm, vm, hb, hb, hb],
        out_specs=[vm, vm, hb, hb, hb],
        scratch_shapes=[
            *[V(v.shape[1:], BF) for v in (gg, gu, gd)],
            *[V(v.shape[1:], F32) for v in (gg, gu, gd)],
            pltpu.SemaphoreType.DMA((3 * parts,)),
            pltpu.SemaphoreType.DMA((3 * parts,)),
        ],
        compiler_params=pltpu.CompilerParams(vmem_limit_bytes=24 * 1024 * 1024),
    )(layer_out, token_grad, gg, gu, gd)


def solution(mesh):
    placed = (
        P(("dp", "ep"), None), P(("dp", "ep"), None), P(("dp", "ep"), None), P(("dp", "ep")), P(),
        P("ep", "dp", None), P("ep", "dp", None), P("ep", "dp", None), P(("dp", "ep"), None),
    )
    return jax.shard_map(
        per_device, mesh=mesh, in_specs=placed,
        out_specs=(
            P(("dp", "ep"), None), P(("dp", "ep"), None),
            P("ep", "dp", None), P("ep", "dp", None), P("ep", "dp", None),
        ),
        check_vma=False,
    )
```

```python
import functools
import jax
import jax.numpy as jnp
from jax import lax
from jax.experimental import pallas as pl
from jax.experimental.pallas import tpu as pltpu
from jax.sharding import PartitionSpec as P

BF = jnp.bfloat16
F32 = jnp.float32
MESH = pl.DeviceIdType.MESH


def dot(a, b, ca, cb):
    return lax.dot_general(a, b, (((ca,), (cb,)), ((), ())), preferred_element_type=F32)


def kernel(
    n_ep, lanes, n_sem,
    bid_hbm, bcnt_hbm, tok_hbm, ids_hbm, quant_hbm, cot_hbm, wg_hbm, wu_hbm, wd_hbm,
    lo_ref, tg_ref, gg_hbm, gu_hbm, gd_hbm,
    gat, wg, wu, wd, og, pa, pb, r1a, r1b, s1a, s1b, r2a, r2b, s2a, s2b, r3a, r3b, s3a, s3b, r4a, r4b,
    ids_v, quant_v, bid_s, bcnt_s, gg, gu, gd,
    send_sems, recv_sems, w_sems, i_sems, o_sems,
):
    R, width = tok_hbm.shape
    top = ids_hbm.shape[1]
    nz = n_ep // 8
    group = 8 * R
    me = lax.axis_index("ep")
    z = me // 8
    rest = me % 8
    y, x, c = rest // 4, (rest // 2) % 2, rest % 2
    base = z * 8
    core_nbr = base + y * 4 + x * 2 + (1 - c)
    x_nbr = base + y * 4 + (1 - x) * 2 + c
    y_nbr = base + (1 - y) * 4 + x * 2 + c
    near = [jnp.where(z < nz // 2, i, nz - i) for i in range(1, nz)]
    far = near[::-1]

    def z_at(k):
        return lax.rem(z + k, nz) * 8 + rest

    a_cols = slice(0, width + lanes)
    b_cols = slice(width + lanes, 2 * width + lanes)
    mid = width // 2
    end = width + lanes
    cols = {
        "a": a_cols, "b": b_cols, "a0": slice(0, mid), "a1": slice(mid, end),
        "b0": slice(end, end + mid), "b1": slice(end + mid, end + width),
    }

    i_copies = [
        pltpu.make_async_copy(src, dst, i_sems.at[i])
        for i, (src, dst) in enumerate((
            (bid_hbm, bid_s), (bcnt_hbm, bcnt_s), (ids_hbm, ids_v), (quant_hbm, quant_v),
            (tok_hbm, gat.at[0, 0:R, 0:width]), (cot_hbm, gat.at[0, 0:R, b_cols]),
        ))
    ]
    for cp in i_copies:
        cp.start()
    w_copies = [
        pltpu.make_async_copy(src.at[0], dst, w_sems.at[i])
        for i, (src, dst) in enumerate(((wg_hbm, wg), (wu_hbm, wu), (wd_hbm, wd)))
    ]
    for cp in w_copies:
        cp.start()
    barrier = pltpu.get_barrier_semaphore()
    for d in [z_at(k) for k in range(1, nz)] + [core_nbr, x_nbr, y_nbr]:
        pl.semaphore_signal(barrier, inc=1, device_id={"ep": d}, device_id_type=MESH)
    for cp in i_copies:
        cp.wait()

    lane = lax.broadcasted_iota(jnp.int32, (R, lanes), 1)
    row = lax.broadcasted_iota(jnp.int32, (R, lanes), 0)
    count = jnp.zeros((R, lanes), jnp.int32)
    for t in range(R):
        count = jnp.where(row == t, bcnt_s[bid_s[t]], count)
    ids = ids_v[...]
    quant = quant_v[...]
    meta = jnp.where(lane == 2 * n_ep, count >> 5, jnp.where(lane == 2 * n_ep + 1, count & 31, 0))
    for k in range(top):
        ik = ids[:, k:k + 1]
        qk = quant[:, k:k + 1]
        meta = meta + jnp.where(lane == ik, qk >> 5, 0) + jnp.where(lane == ik + n_ep, qk & 31, 0)
    gat[0, 0:R, width:width + lanes] = meta.astype(F32).astype(BF)
    pl.semaphore_wait(barrier, nz + 2)

    pending = []
    bases = {}

    def index(name, k):
        if name not in bases:
            bases[name] = len(bases) * nz
        return bases[name] + k

    def send(name, src, dst, target, k):
        i = index(name, k)
        cp = pltpu.make_async_remote_copy(
            src_ref=src, dst_ref=dst, send_sem=send_sems.at[i], recv_sem=recv_sems.at[i],
            device_id={"ep": target}, device_id_type=MESH,
        )
        cp.start()
        pending.append(cp)

    def landed(name, dst, k):
        i = index(name, k)
        pltpu.make_async_remote_copy(
            src_ref=dst, dst_ref=dst, send_sem=send_sems.at[i], recv_sem=recv_sems.at[i],
            device_id={"ep": core_nbr}, device_id_type=MESH,
        ).wait_recv()

    def blk(h, k, cc, yy, xx):
        s = cc * 4 * R + yy * 2 * R + xx * R
        return gat.at[k, s:s + R, cols[h]]

    def to_x(h, k):
        send("x" + h, blk(h, k, 0, 0, 0), blk(h, k, 0, 0, 1), x_nbr, k)

    def to_y(h, k):
        send("y" + h, blk(h, k, 0, 0, 0), blk(h, k, 0, 1, 0), y_nbr, k)

    def to_core(h, k, yy, xx):
        send("c%d%d" % (yy, xx) + h, blk(h, k, 0, yy, xx), blk(h, k, 1, yy, xx), core_nbr, k)

    def spread(h, k):
        if h == "a":
            to_y(h, k)
            to_x(h, k)
        else:
            to_x(h, k)
            to_y(h, k)
        to_core(h, k, 0, 0)

    def start_z(h):
        for k in far:
            send("z" + h, blk(h, 0, 0, 0, 0), blk(h, nz - k, 0, 0, 0), z_at(k), nz - k)

    def pass_z(h, k):
        landed("z" + h, blk(h, k, 0, 0, 0), k)
        spread(h, k)

    def pass_xy(h, k):
        landed("y" + h, blk(h, k, 0, 1, 0), k)
        send("d0" + h, blk(h + "0", k, 0, 1, 0), blk(h + "0", k, 0, 1, 1), x_nbr, k)
        to_core(h, k, 1, 0)
        landed("x" + h, blk(h, k, 0, 0, 1), k)
        send("d1" + h, blk(h + "1", k, 0, 0, 1), blk(h + "1", k, 0, 1, 1), y_nbr, k)
        to_core(h, k, 0, 1)

    def pass_d(h, k):
        landed("d0" + h, blk(h + "0", k, 0, 1, 1), k)
        landed("d1" + h, blk(h + "1", k, 0, 1, 1), k)
        to_core(h, k, 1, 1)

    def all_core(h):
        for k in range(nz):
            for yy in range(2):
                for xx in range(2):
                    landed("c%d%d" % (yy, xx) + h, blk(h, k, 1, yy, xx), k)

    start_z("a")
    spread("a", 0)
    start_z("b")
    spread("b", 0)
    pass_xy("a", 0)
    for k in near:
        pass_z("a", k)
    pass_xy("b", 0)
    for k in near:
        pass_z("b", k)
    for k in near:
        pass_xy("a", k)
    pass_d("a", 0)
    for k in near:
        pass_xy("b", k)
    for k in near:
        pass_d("a", k)
    for cp in w_copies:
        cp.wait()
    all_core("a")

    total = n_ep * R
    toks = gat[:, :, 0:width].reshape(total, width)
    m = gat[:, :, width:width + lanes].reshape(total, lanes).astype(F32)
    ml = lax.broadcasted_iota(jnp.int32, m.shape, 1)
    share = jnp.sum(jnp.where(ml == me, m * 32.0, jnp.where(ml == me + n_ep, m, 0.0)), axis=1, keepdims=True) / 1024.0
    cnt = jnp.sum(jnp.where(ml == 2 * n_ep, m * 32.0, jnp.where(ml == 2 * n_ep + 1, m, 0.0)), axis=1, keepdims=True)
    scale = share * (64.0 / (64.0 + cnt))
    pre_gate = dot(toks, wg[...], 1, 0)
    pre_up = dot(toks, wu[...], 1, 0)
    pass_d("b", 0)
    for k in near:
        pass_d("b", k)
    sig = jax.nn.sigmoid(pre_gate)
    act = pre_gate * sig
    hidden = (act * pre_up).astype(BF)
    pa[...] = (share * dot(hidden, wd[...], 1, 0)).astype(BF).reshape(pa.shape)
    order = far + [0]

    def send1(h, p, r1):
        for k in order:
            send("r1" + h, p.at[k, 4 * R:8 * R, :], r1.at[k], core_nbr, k)

    send1("a", pa, r1a)
    all_core("b")
    og[...] = (scale * gat[:, :, b_cols].reshape(total, width).astype(F32)).astype(BF)
    hg = dot(og[...], wd[...], 1, 1)
    gate_pre = (hg * pre_up * (sig * (1.0 + pre_gate * (1.0 - sig)))).astype(BF)
    up_pre = (hg * act).astype(BF)

    def sub(ref, k, yy, xx):
        s = yy * 2 * R + xx * R
        return ref[k, s:s + R, :].astype(F32)

    left, right = slice(0, mid), slice(mid, width)

    def one(k, yy, xx, p, r1):
        return sub(p, k, yy, xx) + sub(r1, k, yy, xx)

    def step2(h, p, r1, s1, r2):
        for k in order:
            landed("r1" + h, r1.at[k], k)
            corner = one(k, 1, 1, p, r1).astype(BF)
            s1[k, 0:R, left] = one(k, 0, 1, p, r1)[:, left].astype(BF)
            s1[k, R:2 * R, left] = corner[:, left]
            s1[k, 0:R, right] = one(k, 1, 0, p, r1)[:, right].astype(BF)
            s1[k, R:2 * R, right] = corner[:, right]
            send("r2x" + h, s1.at[k, :, left], r2.at[k, :, left], x_nbr, k)
            send("r2y" + h, s1.at[k, :, right], r2.at[k, :, right], y_nbr, k)

    def step3(h, p, r1, r2, s2, r3):
        for k in order:
            landed("r2x" + h, r2.at[k, :, left], k)
            landed("r2y" + h, r2.at[k, :, right], k)
            away = r2[k, R:2 * R, :].astype(F32)
            s2[k, :, left] = (one(k, 1, 0, p, r1)[:, left] + away[:, left]).astype(BF)
            s2[k, :, right] = (one(k, 0, 1, p, r1)[:, right] + away[:, right]).astype(BF)
            send("r3y" + h, s2.at[k, :, left], r3.at[k, :, left], y_nbr, k)
            send("r3x" + h, s2.at[k, :, right], r3.at[k, :, right], x_nbr, k)

    def landed3(h, r3, k):
        landed("r3y" + h, r3.at[k, :, left], k)
        landed("r3x" + h, r3.at[k, :, right], k)

    def local(k, p, r1, r2, r3):
        return one(k, 0, 0, p, r1) + r2[k, 0:R, :].astype(F32) + r3[k].astype(F32)

    def step4(h, p, r1, r2, r3, s3, r4):
        for k in far:
            landed3(h, r3, k)
            s3[k] = local(k, p, r1, r2, r3).astype(BF)
            send("r4" + h, s3.at[k], r4.at[nz - k], z_at(k), nz - k)
        landed3(h, r3, 0)

    def finish(h, p, r1, r2, r3, r4, out_ref):
        acc = local(0, p, r1, r2, r3)
        for k in near:
            landed("r4" + h, r4.at[k], k)
            acc = acc + r4[k].astype(F32)
        out_ref[...] = acc.astype(BF)

    o_copies = []

    def weight_grad(lhs, rhs, buf, out):
        buf[...] = dot(lhs, rhs, 0, 0).astype(BF)
        cp = pltpu.make_async_copy(buf, out.at[0], o_sems.at[len(o_copies)])
        cp.start()
        o_copies.append(cp)

    step2("a", pa, r1a, s1a, r2a)
    pb[...] = (dot(gate_pre, wg[...], 1, 1) + dot(up_pre, wu[...], 1, 1)).astype(BF).reshape(pb.shape)
    send1("b", pb, r1b)
    weight_grad(toks, gate_pre, gg, gg_hbm)
    step2("b", pb, r1b, s1b, r2b)
    step3("a", pa, r1a, r2a, s2a, r3a)
    weight_grad(toks, up_pre, gu, gu_hbm)
    step3("b", pb, r1b, r2b, s2b, r3b)
    step4("a", pa, r1a, r2a, r3a, s3a, r4a)
    weight_grad(hidden, og[...], gd, gd_hbm)
    step4("b", pb, r1b, r2b, r3b, s3b, r4b)
    finish("a", pa, r1a, r2a, r3a, r4a, lo_ref)
    finish("b", pb, r1b, r2b, r3b, r4b, tg_ref)
    for cp in pending:
        cp.wait_send()
    for cp in o_copies:
        cp.wait()
    assert len(bases) * nz == n_sem


def widen(parts, lo_in, tg_in, gg_in, gu_in, gd_in, lo, tg, gg, gu, gd, gb, ub, db, gf, uf, df, in_sems, out_sems):
    lo[...] = lo_in[...]
    tg[...] = tg_in[...]
    work = []
    for w, (src, mid, wide, dst) in enumerate(((gg_in, gb, gf, gg), (gu_in, ub, uf, gu), (gd_in, db, df, gd))):
        rows = mid.shape[0] // parts
        for i in range(parts):
            at = slice(i * rows, (i + 1) * rows)
            n = w * parts + i
            cp = pltpu.make_async_copy(src.at[0, at, :], mid.at[at, :], in_sems.at[n])
            cp.start()
            out = pltpu.make_async_copy(wide.at[at, :], dst.at[0, at, :], out_sems.at[n])
            work.append((cp, out, mid, wide, at))
    for cp, out, mid, wide, at in work:
        cp.wait()
        wide[at, :] = mid[at, :].astype(F32)
        out.start()
    for item in work:
        item[1].wait()


def per_device(
    tokens, expert_ids, gate_quant, bucket_ids, bucket_counts,
    gate_weight, up_weight, down_weight, cotangent,
):
    n_ep = lax.axis_size("ep")
    n_dp = lax.axis_size("dp")
    rows, width = tokens.shape
    if n_dp > 1:
        gate_weight, up_weight, down_weight = (
            lax.all_gather(w, "dp", axis=1, tiled=True)
            for w in (gate_weight, up_weight, down_weight)
        )
    ff = gate_weight.shape[2]
    nz = n_ep // 8
    lanes = -(-(2 * n_ep + 2) // 128) * 128
    n_sem = 30 * nz
    vm = pl.BlockSpec(memory_space=pltpu.VMEM)
    hb = pl.BlockSpec(memory_space=pltpu.HBM)
    V = pltpu.VMEM
    pair = lambda shape: [V(shape, BF), V(shape, BF)]
    outs = pl.pallas_call(
        functools.partial(kernel, n_ep, lanes, n_sem),
        out_shape=(
            jax.ShapeDtypeStruct((rows, width), BF),
            jax.ShapeDtypeStruct((rows, width), BF),
            jax.ShapeDtypeStruct((1, width, ff), BF),
            jax.ShapeDtypeStruct((1, width, ff), BF),
            jax.ShapeDtypeStruct((1, ff, width), BF),
        ),
        in_specs=[hb] * 9,
        out_specs=[vm, vm, hb, hb, hb],
        scratch_shapes=[
            V((nz, 8 * rows, 2 * width + lanes), BF),
            V((width, ff), BF),
            V((width, ff), BF),
            V((ff, width), BF),
            V((n_ep * rows, width), BF),
            *pair((nz, 8 * rows, width)),
            *pair((nz, 4 * rows, width)),
            *pair((nz, 2 * rows, width)),
            *pair((nz, 2 * rows, width)),
            *pair((nz, rows, width)),
            *pair((nz, rows, width)),
            *pair((nz, rows, width)),
            *pair((nz, rows, width)),
            V(expert_ids.shape, jnp.int32),
            V(gate_quant.shape, jnp.int32),
            pltpu.SMEM(bucket_ids.shape, jnp.int32),
            pltpu.SMEM(bucket_counts.shape, jnp.int32),
            V((width, ff), BF),
            V((width, ff), BF),
            V((ff, width), BF),
            pltpu.SemaphoreType.DMA((n_sem,)),
            pltpu.SemaphoreType.DMA((n_sem,)),
            pltpu.SemaphoreType.DMA((3,)),
            pltpu.SemaphoreType.DMA((6,)),
            pltpu.SemaphoreType.DMA((3,)),
        ],
        compiler_params=pltpu.CompilerParams(collective_id=0, has_side_effects=True, vmem_limit_bytes=60 * 1024 * 1024),
    )(bucket_ids, bucket_counts, tokens, expert_ids, gate_quant, cotangent, gate_weight, up_weight, down_weight)
    layer_out, token_grad, gg, gu, gd = outs
    if n_dp > 1:
        gg, gu, gd = (
            lax.psum_scatter(v, "dp", scatter_dimension=1, tiled=True) for v in (gg, gu, gd)
        )
    parts = 2
    wide = [jax.ShapeDtypeStruct(v.shape, F32) for v in (gg, gu, gd)]
    return pl.pallas_call(
        functools.partial(widen, parts),
        out_shape=(
            jax.ShapeDtypeStruct((rows, width), BF),
            jax.ShapeDtypeStruct((rows, width), BF),
            *wide,
        ),
        in_specs=[vm, vm, hb, hb, hb],
        out_specs=[vm, vm, hb, hb, hb],
        scratch_shapes=[
            *[V(v.shape[1:], BF) for v in (gg, gu, gd)],
            *[V(v.shape[1:], F32) for v in (gg, gu, gd)],
            pltpu.SemaphoreType.DMA((3 * parts,)),
            pltpu.SemaphoreType.DMA((3 * parts,)),
        ],
        compiler_params=pltpu.CompilerParams(vmem_limit_bytes=60 * 1024 * 1024),
    )(layer_out, token_grad, gg, gu, gd)


def solution(mesh):
    placed = (
        P(("dp", "ep"), None), P(("dp", "ep"), None), P(("dp", "ep"), None), P(("dp", "ep")), P(),
        P("ep", "dp", None), P("ep", "dp", None), P("ep", "dp", None), P(("dp", "ep"), None),
    )
    return jax.shard_map(
        per_device, mesh=mesh, in_specs=placed,
        out_specs=(
            P(("dp", "ep"), None), P(("dp", "ep"), None),
            P("ep", "dp", None), P("ep", "dp", None), P("ep", "dp", None),
        ),
        check_vma=False,
    )
```

```python
import functools
import jax
import jax.numpy as jnp
from jax import lax
from jax.experimental import pallas as pl
from jax.experimental.pallas import tpu as pltpu
from jax.sharding import PartitionSpec as P

BF = jnp.bfloat16
F32 = jnp.float32
MESH = pl.DeviceIdType.MESH


def dot(a, b, ca, cb):
    return lax.dot_general(a, b, (((ca,), (cb,)), ((), ())), preferred_element_type=F32)


def kernel(
    n_ep, lanes, n_sem,
    bid_hbm, bcnt_hbm, tok_hbm, ids_hbm, quant_hbm, cot_hbm, wg_hbm, wu_hbm, wd_hbm,
    lo_hbm, tg_hbm, gg_hbm, gu_hbm, gd_hbm,
    gat, wg, wu, wd, og, pa, pb, r1a, r1b, s1a, s1b, r2a, r2b, s2a, s2b, r3a, r3b, s3a, s3b, r4a, r4b,
    ids_v, quant_v, bid_s, bcnt_s, gg, gu, gd, lo_v, tg_v,
    send_sems, recv_sems, w_sems, i_sems, o_sems,
):
    R, width = tok_hbm.shape
    top = ids_hbm.shape[1]
    nz = n_ep // 8
    group = 8 * R
    me = lax.axis_index("ep")
    z = me // 8
    rest = me % 8
    y, x, c = rest // 4, (rest // 2) % 2, rest % 2
    base = z * 8
    core_nbr = base + y * 4 + x * 2 + (1 - c)
    x_nbr = base + y * 4 + (1 - x) * 2 + c
    y_nbr = base + (1 - y) * 4 + x * 2 + c
    near = [jnp.where(z < nz // 2, i, nz - i) for i in range(1, nz)]
    far = near[::-1]

    def z_at(k):
        return lax.rem(z + k, nz) * 8 + rest

    a_cols = slice(0, width + lanes)
    b_cols = slice(width + lanes, 2 * width + lanes)
    mid = width // 2
    end = width + lanes
    cols = {
        "a": a_cols, "b": b_cols, "a0": slice(0, mid), "a1": slice(mid, end),
        "b0": slice(end, end + mid), "b1": slice(end + mid, end + width),
    }

    i_copies = [
        pltpu.make_async_copy(src, dst, i_sems.at[i])
        for i, (src, dst) in enumerate((
            (bid_hbm, bid_s), (bcnt_hbm, bcnt_s), (ids_hbm, ids_v), (quant_hbm, quant_v),
            (tok_hbm, gat.at[0, 0:R, 0:width]), (cot_hbm, gat.at[0, 0:R, b_cols]),
        ))
    ]
    for cp in i_copies:
        cp.start()
    w_copies = [
        pltpu.make_async_copy(src.at[0], dst, w_sems.at[i])
        for i, (src, dst) in enumerate(((wg_hbm, wg), (wu_hbm, wu), (wd_hbm, wd)))
    ]
    for cp in w_copies:
        cp.start()
    barrier = pltpu.get_barrier_semaphore()
    for d in [z_at(k) for k in range(1, nz)] + [core_nbr, x_nbr, y_nbr]:
        pl.semaphore_signal(barrier, inc=1, device_id={"ep": d}, device_id_type=MESH)
    for cp in i_copies:
        cp.wait()

    lane = lax.broadcasted_iota(jnp.int32, (R, lanes), 1)
    row = lax.broadcasted_iota(jnp.int32, (R, lanes), 0)
    count = jnp.zeros((R, lanes), jnp.int32)
    for t in range(R):
        count = jnp.where(row == t, bcnt_s[bid_s[t]], count)
    ids = ids_v[...]
    quant = quant_v[...]
    meta = jnp.where(lane == 2 * n_ep, count >> 5, jnp.where(lane == 2 * n_ep + 1, count & 31, 0))
    for k in range(top):
        ik = ids[:, k:k + 1]
        qk = quant[:, k:k + 1]
        meta = meta + jnp.where(lane == ik, qk >> 5, 0) + jnp.where(lane == ik + n_ep, qk & 31, 0)
    gat[0, 0:R, width:width + lanes] = meta.astype(F32).astype(BF)
    pl.semaphore_wait(barrier, nz + 2)

    pending = []
    bases = {}

    def index(name, k):
        if name not in bases:
            bases[name] = len(bases) * nz
        return bases[name] + k

    def send(name, src, dst, target, k):
        i = index(name, k)
        cp = pltpu.make_async_remote_copy(
            src_ref=src, dst_ref=dst, send_sem=send_sems.at[i], recv_sem=recv_sems.at[i],
            device_id={"ep": target}, device_id_type=MESH,
        )
        cp.start()
        pending.append(cp)

    def landed(name, dst, k):
        i = index(name, k)
        pltpu.make_async_remote_copy(
            src_ref=dst, dst_ref=dst, send_sem=send_sems.at[i], recv_sem=recv_sems.at[i],
            device_id={"ep": core_nbr}, device_id_type=MESH,
        ).wait_recv()

    def blk(h, k, cc, yy, xx):
        s = cc * 4 * R + yy * 2 * R + xx * R
        return gat.at[k, s:s + R, cols[h]]

    def to_x(h, k):
        send("x" + h, blk(h, k, 0, 0, 0), blk(h, k, 0, 0, 1), x_nbr, k)

    def to_y(h, k):
        send("y" + h, blk(h, k, 0, 0, 0), blk(h, k, 0, 1, 0), y_nbr, k)

    def to_core(h, k, yy, xx):
        send("c%d%d" % (yy, xx) + h, blk(h, k, 0, yy, xx), blk(h, k, 1, yy, xx), core_nbr, k)

    def spread(h, k):
        if h == "a":
            to_y(h, k)
            to_x(h, k)
        else:
            to_x(h, k)
            to_y(h, k)
        to_core(h, k, 0, 0)

    def start_z(h):
        for k in far:
            send("z" + h, blk(h, 0, 0, 0, 0), blk(h, nz - k, 0, 0, 0), z_at(k), nz - k)

    def pass_z(h, k):
        landed("z" + h, blk(h, k, 0, 0, 0), k)
        spread(h, k)

    def pass_xy(h, k):
        landed("y" + h, blk(h, k, 0, 1, 0), k)
        send("d0" + h, blk(h + "0", k, 0, 1, 0), blk(h + "0", k, 0, 1, 1), x_nbr, k)
        to_core(h, k, 1, 0)
        landed("x" + h, blk(h, k, 0, 0, 1), k)
        send("d1" + h, blk(h + "1", k, 0, 0, 1), blk(h + "1", k, 0, 1, 1), y_nbr, k)
        to_core(h, k, 0, 1)

    def pass_d(h, k):
        landed("d0" + h, blk(h + "0", k, 0, 1, 1), k)
        landed("d1" + h, blk(h + "1", k, 0, 1, 1), k)
        to_core(h, k, 1, 1)

    def all_core(h):
        for k in range(nz):
            for yy in range(2):
                for xx in range(2):
                    landed("c%d%d" % (yy, xx) + h, blk(h, k, 1, yy, xx), k)

    start_z("a")
    spread("a", 0)
    start_z("b")
    spread("b", 0)
    pass_xy("a", 0)
    for k in near:
        pass_z("a", k)
    pass_xy("b", 0)
    for k in near:
        pass_z("b", k)
    for k in near:
        pass_xy("a", k)
    pass_d("a", 0)
    for k in near:
        pass_xy("b", k)
    for k in near:
        pass_d("a", k)
    pass_d("b", 0)
    for k in near:
        pass_d("b", k)
    for cp in w_copies:
        cp.wait()
    all_core("a")

    total = n_ep * R
    toks = gat[:, :, 0:width].reshape(total, width)
    m = gat[:, :, width:width + lanes].reshape(total, lanes).astype(F32)
    ml = lax.broadcasted_iota(jnp.int32, m.shape, 1)
    share = jnp.sum(jnp.where(ml == me, m * 32.0, jnp.where(ml == me + n_ep, m, 0.0)), axis=1, keepdims=True) / 1024.0
    cnt = jnp.sum(jnp.where(ml == 2 * n_ep, m * 32.0, jnp.where(ml == 2 * n_ep + 1, m, 0.0)), axis=1, keepdims=True)
    scale = share * (64.0 / (64.0 + cnt))
    pre_gate = dot(toks, wg[...], 1, 0)
    pre_up = dot(toks, wu[...], 1, 0)
    sig = jax.nn.sigmoid(pre_gate)
    act = pre_gate * sig
    hidden = (act * pre_up).astype(BF)
    pa[...] = (share * dot(hidden, wd[...], 1, 0)).astype(BF).reshape(pa.shape)
    order = far + [0]

    def send1(h, p, r1):
        for k in order:
            send("r1" + h, p.at[k, 4 * R:8 * R, :], r1.at[k], core_nbr, k)

    send1("a", pa, r1a)
    all_core("b")
    og[...] = (scale * gat[:, :, b_cols].reshape(total, width).astype(F32)).astype(BF)
    hg = dot(og[...], wd[...], 1, 1)
    gate_pre = (hg * pre_up * (sig * (1.0 + pre_gate * (1.0 - sig)))).astype(BF)
    up_pre = (hg * act).astype(BF)

    def sub(ref, k, yy, xx):
        s = yy * 2 * R + xx * R
        return ref[k, s:s + R, :].astype(F32)

    left, right = slice(0, mid), slice(mid, width)

    def one(k, yy, xx, p, r1):
        return sub(p, k, yy, xx) + sub(r1, k, yy, xx)

    def step2(h, p, r1, s1, r2):
        for k in order:
            landed("r1" + h, r1.at[k], k)
            corner = one(k, 1, 1, p, r1).astype(BF)
            s1[k, 0:R, left] = one(k, 0, 1, p, r1)[:, left].astype(BF)
            s1[k, R:2 * R, left] = corner[:, left]
            s1[k, 0:R, right] = one(k, 1, 0, p, r1)[:, right].astype(BF)
            s1[k, R:2 * R, right] = corner[:, right]
            send("r2x" + h, s1.at[k, :, left], r2.at[k, :, left], x_nbr, k)
            send("r2y" + h, s1.at[k, :, right], r2.at[k, :, right], y_nbr, k)

    def step3(h, p, r1, r2, s2, r3):
        for k in order:
            landed("r2x" + h, r2.at[k, :, left], k)
            landed("r2y" + h, r2.at[k, :, right], k)
            away = r2[k, R:2 * R, :].astype(F32)
            s2[k, :, left] = (one(k, 1, 0, p, r1)[:, left] + away[:, left]).astype(BF)
            s2[k, :, right] = (one(k, 0, 1, p, r1)[:, right] + away[:, right]).astype(BF)
            send("r3y" + h, s2.at[k, :, left], r3.at[k, :, left], y_nbr, k)
            send("r3x" + h, s2.at[k, :, right], r3.at[k, :, right], x_nbr, k)

    def landed3(h, r3, k):
        landed("r3y" + h, r3.at[k, :, left], k)
        landed("r3x" + h, r3.at[k, :, right], k)

    def local(k, p, r1, r2, r3):
        return one(k, 0, 0, p, r1) + r2[k, 0:R, :].astype(F32) + r3[k].astype(F32)

    def step4(h, p, r1, r2, r3, s3, r4):
        for k in far:
            landed3(h, r3, k)
            s3[k] = local(k, p, r1, r2, r3).astype(BF)
            send("r4" + h, s3.at[k], r4.at[nz - k], z_at(k), nz - k)
        landed3(h, r3, 0)

    def finish(h, p, r1, r2, r3, r4, buf, out):
        acc = local(0, p, r1, r2, r3)
        for k in near:
            landed("r4" + h, r4.at[k], k)
            acc = acc + r4[k].astype(F32)
        buf[...] = acc.astype(BF)
        cp = pltpu.make_async_copy(buf, out, o_sems.at[len(o_copies)])
        cp.start()
        o_copies.append(cp)

    o_copies = []

    def weight_grad(lhs, rhs, buf, out):
        buf[...] = dot(lhs, rhs, 0, 0).astype(BF)
        cp = pltpu.make_async_copy(buf, out.at[0], o_sems.at[len(o_copies)])
        cp.start()
        o_copies.append(cp)

    step2("a", pa, r1a, s1a, r2a)
    pb[...] = (dot(gate_pre, wg[...], 1, 1) + dot(up_pre, wu[...], 1, 1)).astype(BF).reshape(pb.shape)
    send1("b", pb, r1b)
    weight_grad(toks, gate_pre, gg, gg_hbm)
    step2("b", pb, r1b, s1b, r2b)
    step3("a", pa, r1a, r2a, s2a, r3a)
    weight_grad(toks, up_pre, gu, gu_hbm)
    step3("b", pb, r1b, r2b, s2b, r3b)
    step4("a", pa, r1a, r2a, r3a, s3a, r4a)
    weight_grad(hidden, og[...], gd, gd_hbm)
    step4("b", pb, r1b, r2b, r3b, s3b, r4b)
    finish("a", pa, r1a, r2a, r3a, r4a, lo_v, lo_hbm)
    finish("b", pb, r1b, r2b, r3b, r4b, tg_v, tg_hbm)
    for cp in pending:
        cp.wait_send()
    for cp in o_copies:
        cp.wait()
    assert len(bases) * nz == n_sem


def widen(parts, lo_in, tg_in, gg_in, gu_in, gd_in, lo, tg, gg, gu, gd, lb, tb, gb, ub, db, gf, uf, df, in_sems, out_sems):
    work = []
    small = []
    for w, (src, mid, wide, dst) in enumerate(((gg_in, gb, gf, gg), (gu_in, ub, uf, gu), (gd_in, db, df, gd))):
        rows = mid.shape[0] // parts
        for i in range(parts):
            at = slice(i * rows, (i + 1) * rows)
            n = w * parts + i
            cp = pltpu.make_async_copy(src.at[0, at, :], mid.at[at, :], in_sems.at[n])
            cp.start()
            out = pltpu.make_async_copy(wide.at[at, :], dst.at[0, at, :], out_sems.at[n])
            work.append((cp, out, mid, wide, at))
    for i, (src, mid, dst) in enumerate(((lo_in, lb, lo), (tg_in, tb, tg))):
        cp = pltpu.make_async_copy(src, mid, in_sems.at[3 * parts + i])
        cp.start()
        small.append((cp, pltpu.make_async_copy(mid, dst, out_sems.at[3 * parts + i])))
    for cp, out, mid, wide, at in work:
        cp.wait()
        wide[at, :] = mid[at, :].astype(F32)
        out.start()
    for cp, out in small:
        cp.wait()
        out.start()
    for item in work + small:
        item[1].wait()


def per_device(
    tokens, expert_ids, gate_quant, bucket_ids, bucket_counts,
    gate_weight, up_weight, down_weight, cotangent,
):
    n_ep = lax.axis_size("ep")
    n_dp = lax.axis_size("dp")
    rows, width = tokens.shape
    if n_dp > 1:
        gate_weight, up_weight, down_weight = (
            lax.all_gather(w, "dp", axis=1, tiled=True)
            for w in (gate_weight, up_weight, down_weight)
        )
    ff = gate_weight.shape[2]
    nz = n_ep // 8
    lanes = -(-(2 * n_ep + 2) // 128) * 128
    n_sem = 30 * nz
    hb = pl.BlockSpec(memory_space=pltpu.HBM)
    V = pltpu.VMEM
    pair = lambda shape: [V(shape, BF), V(shape, BF)]
    outs = pl.pallas_call(
        functools.partial(kernel, n_ep, lanes, n_sem),
        out_shape=(
            jax.ShapeDtypeStruct((rows, width), BF),
            jax.ShapeDtypeStruct((rows, width), BF),
            jax.ShapeDtypeStruct((1, width, ff), BF),
            jax.ShapeDtypeStruct((1, width, ff), BF),
            jax.ShapeDtypeStruct((1, ff, width), BF),
        ),
        in_specs=[hb] * 9,
        out_specs=[hb] * 5,
        scratch_shapes=[
            V((nz, 8 * rows, 2 * width + lanes), BF),
            V((width, ff), BF),
            V((width, ff), BF),
            V((ff, width), BF),
            V((n_ep * rows, width), BF),
            *pair((nz, 8 * rows, width)),
            *pair((nz, 4 * rows, width)),
            *pair((nz, 2 * rows, width)),
            *pair((nz, 2 * rows, width)),
            *pair((nz, rows, width)),
            *pair((nz, rows, width)),
            *pair((nz, rows, width)),
            *pair((nz, rows, width)),
            V(expert_ids.shape, jnp.int32),
            V(gate_quant.shape, jnp.int32),
            pltpu.SMEM(bucket_ids.shape, jnp.int32),
            pltpu.SMEM(bucket_counts.shape, jnp.int32),
            V((width, ff), BF),
            V((width, ff), BF),
            V((ff, width), BF),
            *pair((rows, width)),
            pltpu.SemaphoreType.DMA((n_sem,)),
            pltpu.SemaphoreType.DMA((n_sem,)),
            pltpu.SemaphoreType.DMA((3,)),
            pltpu.SemaphoreType.DMA((6,)),
            pltpu.SemaphoreType.DMA((5,)),
        ],
        compiler_params=pltpu.CompilerParams(collective_id=0, has_side_effects=True, vmem_limit_bytes=60 * 1024 * 1024),
    )(bucket_ids, bucket_counts, tokens, expert_ids, gate_quant, cotangent, gate_weight, up_weight, down_weight)
    layer_out, token_grad, gg, gu, gd = outs
    if n_dp > 1:
        gg, gu, gd = (
            lax.psum_scatter(v, "dp", scatter_dimension=1, tiled=True) for v in (gg, gu, gd)
        )
    parts = 2
    wide = [jax.ShapeDtypeStruct(v.shape, F32) for v in (gg, gu, gd)]
    return pl.pallas_call(
        functools.partial(widen, parts),
        out_shape=(
            jax.ShapeDtypeStruct((rows, width), BF),
            jax.ShapeDtypeStruct((rows, width), BF),
            *wide,
        ),
        in_specs=[hb] * 5,
        out_specs=[hb] * 5,
        scratch_shapes=[
            *pair((rows, width)),
            *[V(v.shape[1:], BF) for v in (gg, gu, gd)],
            *[V(v.shape[1:], F32) for v in (gg, gu, gd)],
            pltpu.SemaphoreType.DMA((3 * parts + 2,)),
            pltpu.SemaphoreType.DMA((3 * parts + 2,)),
        ],
        compiler_params=pltpu.CompilerParams(vmem_limit_bytes=60 * 1024 * 1024),
    )(layer_out, token_grad, gg, gu, gd)


def solution(mesh):
    placed = (
        P(("dp", "ep"), None), P(("dp", "ep"), None), P(("dp", "ep"), None), P(("dp", "ep")), P(),
        P("ep", "dp", None), P("ep", "dp", None), P("ep", "dp", None), P(("dp", "ep"), None),
    )
    return jax.shard_map(
        per_device, mesh=mesh, in_specs=placed,
        out_specs=(
            P(("dp", "ep"), None), P(("dp", "ep"), None),
            P("ep", "dp", None), P("ep", "dp", None), P("ep", "dp", None),
        ),
        check_vma=False,
    )
```
